32 devices in a mesh: dp: 8 (over z, x), mp: 4 (over y, core).
Axes of the slice: x: 2, y: 2, z: 4, core: 2. Of those that a mesh axis runs over, the one named last changes fastest.
Arguments:
- sparse_vecs: bfloat16 [8192, 26, 128], P(('dp', 'mp')), may hold values from -6 to 6
- dense_vec: bfloat16 [8192, 128], P(('dp', 'mp')), may hold values from -6 to 6
- top_cot: bfloat16 [8192, 1024], P(('dp', 'mp')), may hold values from -0.59765625 to 0.59765625
- top_weight: bfloat16 [479, 1024], replicated, may hold values from -0.25 to 0.25
- owner_ids: int32 [8192, 26, 1], P(('dp', 'mp')), may hold values from 0 to 7; in each aligned block of 6656 rows (0 to 6655, 6656 to 13311, ..., all dimensions but the last counted through in order) at most 1664 rows name the same one
- local_rows: int32 [8192, 26], P(('dp', 'mp')), may hold values from 0 to 127
- table: float32 [26, 1024, 128], P(None, ('dp', 'mp')), may hold values from -0.6 to 0.6
- accum: float32 [26, 1024], P(None, ('dp', 'mp')), may hold values from 0.05 to 2
Outputs:
- dense_grad: bfloat16 [8192, 128], P(('dp', 'mp'))
- new_table: float32 [26, 1024, 128], P(None, ('dp', 'mp'))
- new_accum: float32 [26, 1024], P(None, ('dp', 'mp'))
The draws below stay inside these ranges and needn't reach their ends.
Inputs may be any that keep to these rules, and one draw needn't show every extreme that they name: `owner_ids`: among the lookups of one device's 256 samples no owner group is named more than 1664 times; in every draw some device names some owner group exactly 1664 times.
All inputs are finite; a program needn't handle non-finite values.
Results may differ from the reference program's by a relative error of at most 0.005.
Values may be sent and summed in bfloat16 or wider, within the bound.
No kernel may reach another device: no remote copies, remote signals or barrier semaphores. Data moves between devices by JAX's collectives and lax.ppermute only.
A program may use at most 128 MiB of HBM per device.

```python
import math
import jax
import jax.numpy as jnp
import numpy as np
from jax import lax

E = 128
TABLES = 26
H1 = 1024
B_DEV = 256
ZIN = 479
BATCH = 8192
LOOK_DEV = 6656
ROWS_GRP = 128
ROWS = 1024
CAP = 1664
N_DP = 8


def with_ends(drawn, rng, low, high):
    place = [jax.random.randint(jax.random.fold_in(rng, axis), (), 0, length) for axis, length in enumerate(drawn.shape)]
    main_axis = drawn.shape.index(max(drawn.shape))
    next_to = place[:main_axis] + [(place[main_axis] + 1) % drawn.shape[main_axis]] + place[main_axis + 1:]
    return drawn.at[tuple(place)].set(low).at[tuple(next_to)].set(high)


def shard_levels(key, extent, pieces, low, largest):
    def one(axis_at, shards_of):
        steps = jax.random.uniform(jax.random.fold_in(jax.random.fold_in(key, 6), axis_at), (shards_of,), jnp.float32, low / len(pieces), largest / len(pieces))
        return jnp.repeat(jnp.exp(steps), extent[axis_at] // shards_of).reshape((-1,) + (1,) * (len(extent) - axis_at - 1))

    gain = one(*pieces[0])
    for cut in pieces[1:]:
        gain = gain * one(*cut)
    return gain


def rank_bounds(count, lean):
    loads = [(1 << 20) // math.isqrt(standing ** lean) + 1 for standing in range(1, count + 1)]
    spread = 1 + sum(loads) // (1 << 30)
    return np.cumsum(np.array([max(1, weight // spread) for weight in loads]))


def ranked(key, dims, amount, lean):
    listing = rank_bounds(amount, lean)
    ticket = jax.random.randint(jax.random.fold_in(key, 1), dims, 0, int(listing[amount - 1]))
    standing = jnp.searchsorted(jnp.asarray(listing, jnp.int32), ticket, side="right")
    return jax.random.permutation(jax.random.fold_in(key, 2), amount)[standing].astype(jnp.int32)


def shared_out(own_key, own, number, rows, number_of, top, most, slope):
    order = jax.random.permutation(own_key, number_of)
    heavy_load, usual = load_shares(number_of, rows * top, most, slope, True), load_shares(number_of, rows * top, most, slope, False)
    places = jnp.arange(number_of)

    def named(sizes, rotation):
        used = int((sizes > 0).sum())
        fixed = max(1, used // 4)
        moved = fixed + (places - fixed + rotation * (used - fixed)) % max(1, number_of - fixed)
        return jnp.zeros((number_of,), jnp.int32).at[order[jnp.where(places < fixed, places, moved)]].set(jnp.asarray(sizes, jnp.int32))

    sizes = jnp.where(number % 4 == 0, named(heavy_load, number // 4), named(usual, number - number // 4 - 1))
    mixed = jax.random.permutation(jax.random.fold_in(own, 3), number_of)
    donor, taker = mixed[0:number_of // 2 * 2:2], mixed[1:number_of // 2 * 2:2]
    room = jnp.minimum(sizes[donor] - 1, most - sizes[taker]) // 2
    room = jnp.where((donor == order[0]) | (taker == order[0]) | (sizes[taker] == 0), 0, jnp.maximum(room, 0))
    moved = jax.random.randint(jax.random.fold_in(own, 4), (number_of // 2,), 0, 1 << 20) % (room + 1)
    sizes = sizes.at[donor].add(-moved).at[taker].add(moved)
    members = jnp.searchsorted(jnp.cumsum(sizes), jnp.arange(rows * top), side="right").astype(jnp.int32)
    table = members.reshape(top, rows).T
    table = table[jax.random.permutation(jax.random.fold_in(own, 1), rows)]
    rotation = jax.random.randint(jax.random.fold_in(own, 2), (rows, 1), 0, top)
    return jnp.take_along_axis(table, (jnp.arange(top)[None, :] + rotation) % top, axis=1)


def load_shares(amount, total, most, lean, full):
    loads = [(1 << 20) // math.isqrt(grade ** lean) + 1 for grade in range(1, amount + 1)]
    largest = most if full else min(most, max(-(-total // amount), total * loads[0] // sum(loads)))
    least = 1 if total - largest >= amount - 1 else 0
    counts, surplus = [largest] + [least] * (amount - 1), total - largest - least * (amount - 1)
    while surplus > 0:
        free = [i for i in range(1, amount) if counts[i] < largest] or [i for i in range(1, amount) if counts[i] < most]
        pool, budget = sum([loads[i] for i in free]), surplus
        for i in free:
            more = min(most - counts[i], max(1, budget * loads[i] // pool), surplus)
            counts[i] = counts[i] + more
            surplus = surplus - more
    return np.array(counts)


def scatter_about(key, dims, scale, most, shards=(), kind=jnp.bfloat16):
    level = shard_levels(key, dims, shards, -0.22, 0.18) if shards else 1.0
    array = jax.random.normal(key, dims, jnp.float32) * scale * level
    return jnp.minimum(jnp.maximum(array, -most), most).astype(kind)


def setup_inputs(seed: int = 0) -> dict:
    seeds = jax.random.split(jax.random.key(seed), 9)
    sparse_vecs = scatter_about(seeds[0], (BATCH, TABLES, E), 1.0, 6.0, ((0, 32),))
    dense_vec = scatter_about(seeds[1], (BATCH, E), 1.0, 6.0, ((0, 32),))
    top_cot = scatter_about(seeds[2], (BATCH, H1), 0.1, 0.59765625, ((0, 32),))
    top_weight = scatter_about(seeds[3], (ZIN, H1), ZIN ** -0.5, 0.25)
    owner_ids_keys = jax.random.split(jax.random.fold_in(seeds[4], 1), BATCH * TABLES // LOOK_DEV)
    owner_ids_turns = jax.random.permutation(jax.random.fold_in(seeds[4], 3), BATCH * TABLES // LOOK_DEV)
    owner_ids = jax.vmap(lambda own, number: shared_out(jax.random.fold_in(seeds[4], 2), own, number, LOOK_DEV, N_DP, 1, CAP, 1))(owner_ids_keys, owner_ids_turns).reshape((BATCH, TABLES, 1))
    local_rows = with_ends(ranked(seeds[5], (BATCH, TABLES), ROWS_GRP, 2), jax.random.fold_in(seeds[5], 3), 0, ROWS_GRP - 1).astype(jnp.int32)
    table = scatter_about(seeds[6], (TABLES, ROWS, E), 0.1, 0.6, ((1, 32),), jnp.float32)
    accum = jnp.clip(jnp.exp(math.log(2.0) - 3.6888794 * jax.random.uniform(seeds[7], (TABLES, ROWS), jnp.float32) ** shard_levels(seeds[7], (TABLES, ROWS), ((1, 32),), -0.2, 0.2)), 0.05, 2.0)
    return dict(sparse_vecs=sparse_vecs, dense_vec=dense_vec, top_cot=top_cot, top_weight=top_weight, owner_ids=owner_ids, local_rows=local_rows, table=table, accum=accum)


LEARN_RATE = 0.1
EPSILON = 1e-08

def pair_matrix(feature_count):
    row_index, col_index = np.tril_indices(feature_count, -1)
    pair_count = row_index.shape[0]
    matrix = np.zeros((pair_count, feature_count * feature_count), np.float32)
    matrix[np.arange(pair_count), row_index * feature_count + col_index] = 1.0
    matrix[np.arange(pair_count), col_index * feature_count + row_index] = 1.0
    return matrix

def interaction(sparse_vecs, dense_vec, top_cot, top_weight):
    batch_rows, table_count, row_width = sparse_vecs.shape
    feature_count = table_count + 1
    input_cot = jnp.dot(top_cot, top_weight.T, preferred_element_type=jnp.float32)
    symmetric = jnp.dot(input_cot[:, row_width:], pair_matrix(feature_count), precision=lax.Precision.HIGHEST)
    symmetric = symmetric.reshape(batch_rows, feature_count, feature_count)
    features = jnp.concatenate([dense_vec[:, None, :], sparse_vecs], axis=1).astype(jnp.float32)
    feature_grad = jnp.einsum('bij,bje->bie', symmetric, features, precision=lax.Precision.HIGHEST)
    dense_grad = (input_cot[:, :row_width] + feature_grad[:, 0]).astype(jnp.bfloat16)
    sparse_grad = feature_grad[:, 1:].astype(jnp.bfloat16)
    return (dense_grad, sparse_grad)

def reference(sparse_vecs, dense_vec, top_cot, top_weight, owner_ids, local_rows, table, accum):
    block_count = BATCH // B_DEV

    def one_block(blocks):
        return interaction(blocks[0], blocks[1], blocks[2], top_weight)
    dense_grad, sparse_grad = lax.map(one_block, (sparse_vecs.reshape(block_count, B_DEV, TABLES, E), dense_vec.reshape(block_count, B_DEV, E), top_cot.reshape(block_count, B_DEV, H1)))
    dense_grad = dense_grad.reshape(BATCH, E)
    sparse_grad = sparse_grad.reshape(BATCH, TABLES, E)
    row_total = ROWS_GRP * N_DP
    row_keys = jnp.arange(TABLES, dtype=jnp.int32)[None, :] * row_total + owner_ids[:, :, 0] * ROWS_GRP + local_rows
    row_grad = jax.ops.segment_sum(sparse_grad.astype(jnp.float32).reshape(BATCH * TABLES, E), row_keys.reshape(BATCH * TABLES).astype(jnp.int32), num_segments=TABLES * row_total)
    row_grad = row_grad.reshape(TABLES, row_total, E)
    new_accum = accum + lax.optimization_barrier(jnp.mean(row_grad * row_grad, axis=-1))
    new_table = table - LEARN_RATE * row_grad / (jnp.sqrt(new_accum)[:, :, None] + EPSILON)
    return (dense_grad, new_table, new_accum)
```

```python
import jax
import jax.numpy as jnp
import numpy as np
from jax import lax
from jax.experimental import pallas as pl
from jax.experimental.pallas import tpu as pltpu
from jax.sharding import PartitionSpec as P

LEARN_RATE = 0.1
EPSILON = 1e-08


def symmetric_rows(feature_count):
    row_index, col_index = np.tril_indices(feature_count, -1)
    pair_count = row_index.shape[0]
    matrix = np.zeros((feature_count, feature_count, pair_count), np.float32)
    matrix[row_index, col_index, np.arange(pair_count)] = 1.0
    matrix[col_index, row_index, np.arange(pair_count)] = 1.0
    return jnp.asarray(matrix.reshape(feature_count * feature_count, pair_count), jnp.bfloat16)


def interaction(sparse_vecs, dense_vec, top_cot, top_weight):
    batch_rows, table_count, row_width = sparse_vecs.shape
    feature_count = table_count + 1
    expanded = jnp.dot(
        symmetric_rows(feature_count), top_weight[row_width:], preferred_element_type=jnp.float32
    ).astype(jnp.bfloat16)
    direct = jnp.einsum(
        "bh,zh->bz", top_cot, top_weight[:row_width], preferred_element_type=jnp.float32
    )
    symmetric = jnp.einsum("bh,zh->bz", top_cot, expanded, preferred_element_type=jnp.float32)
    symmetric = symmetric.reshape(batch_rows, feature_count, feature_count)
    features = jnp.concatenate([dense_vec[:, None, :], sparse_vecs], axis=1).astype(jnp.float32)
    feature_grad = jnp.einsum("bij,bje->bie", symmetric, features, precision=lax.Precision.HIGHEST)
    dense_grad = (direct + feature_grad[:, 0]).astype(jnp.bfloat16)
    sparse_grad = feature_grad[:, 1:].astype(jnp.bfloat16)
    return dense_grad, sparse_grad


def sum_kernel(ids_ref, rows_ref, out_ref):
    sources = rows_ref.shape[0]
    blocks, _, block_rows, width = out_ref.shape
    samples = rows_ref.shape[2]
    base = pl.program_id(1) * (blocks * block_rows)
    target = lax.broadcasted_iota(jnp.int32, (blocks * block_rows, samples), 0) + base
    total = jnp.zeros((blocks * block_rows, width), jnp.float32)
    for s in range(sources):
        onehot = (target == ids_ref[s, 0]).astype(jnp.float32).astype(jnp.bfloat16)
        total = total + jnp.dot(onehot, rows_ref[s, 0], preferred_element_type=jnp.float32)
    out_ref[...] = total.reshape(blocks, 1, block_rows, width).astype(out_ref.dtype)


def sum_rows(ids, rows, blocks, block_rows, dtype):
    sources, tables, samples, width = rows.shape
    step = 4 if blocks % 4 == 0 else 1
    return pl.pallas_call(
        sum_kernel,
        grid=(tables, blocks // step),
        in_specs=[
            pl.BlockSpec((sources, 1, 1, samples), lambda t, h: (0, t, 0, 0)),
            pl.BlockSpec((sources, 1, samples, width), lambda t, h: (0, t, 0, 0)),
        ],
        out_specs=pl.BlockSpec((step, 1, block_rows, width), lambda t, h: (h, t, 0, 0)),
        out_shape=jax.ShapeDtypeStruct((blocks, tables, block_rows, width), dtype),
        cost_estimate=pl.CostEstimate(
            flops=2 * tables * sources * samples * blocks * block_rows * width,
            bytes_accessed=rows.size * 2 + blocks * tables * block_rows * width * 4,
            transcendentals=0,
        ),
    )(ids[:, :, None, :], rows)


def per_device(sparse_vecs, dense_vec, top_cot, top_weight, owner_ids, local_rows, table, accum):
    batch_rows, table_count, row_width = sparse_vecs.shape
    dp_count, mp_count = lax.axis_size("dp"), lax.axis_size("mp")
    rows_own = table.shape[1]
    group_rows = rows_own * mp_count
    per_mp = -(-table_count // mp_count)
    padding = per_mp * mp_count - table_count
    inner = 2 if dp_count % 2 == 0 else 1
    outer = dp_count // inner

    keys = (owner_ids[:, :, 0] * group_rows + local_rows).T
    keys = jnp.pad(keys, ((0, padding), (0, 0)), constant_values=-1)
    keys = lax.all_to_all(
        keys.reshape(mp_count, per_mp, batch_rows), "mp", split_axis=0, concat_axis=0, tiled=True
    )

    dense_grad, sparse_grad = interaction(sparse_vecs, dense_vec, top_cot, top_weight)
    send = jnp.pad(sparse_grad.transpose(1, 0, 2), ((0, padding), (0, 0), (0, 0)))
    rows = lax.all_to_all(
        send.reshape(mp_count, per_mp, batch_rows, row_width),
        "mp",
        split_axis=0,
        concat_axis=0,
        tiled=True,
    )

    owner, local = keys // group_rows, keys % group_rows
    place = owner // inner * group_rows + local
    part = owner % inner
    mine = lax.axis_index("dp") % inner
    total = sum_rows(
        jnp.where((keys >= 0) & (part == mine), place, -1), rows, outer, group_rows, jnp.float32
    )
    if inner == 2:
        other = sum_rows(
            jnp.where((keys >= 0) & (part != mine), place, -1),
            rows,
            outer,
            group_rows,
            jnp.bfloat16,
        )
        swap = [(i, i ^ 1) for i in range(dp_count)]
        total = total + lax.ppermute(other, "dp", swap).astype(jnp.float32)
    groups = [[r + inner * k for k in range(outer)] for r in range(inner)]
    parts = lax.all_to_all(
        total.astype(jnp.bfloat16),
        "dp",
        split_axis=0,
        concat_axis=0,
        axis_index_groups=groups,
        tiled=True,
    )
    summed = jnp.sum(parts.astype(jnp.float32), axis=0).astype(jnp.bfloat16)
    summed = summed.reshape(per_mp, mp_count, rows_own, row_width).transpose(1, 0, 2, 3)
    row_grad = lax.all_to_all(summed, "mp", split_axis=0, concat_axis=0, tiled=True)
    row_grad = row_grad.reshape(per_mp * mp_count, rows_own, row_width)[:table_count]
    row_grad = row_grad.astype(jnp.float32)
    new_accum = accum + jnp.mean(row_grad * row_grad, axis=-1)
    new_table = table - LEARN_RATE * row_grad / (jnp.sqrt(new_accum)[:, :, None] + EPSILON)
    return (dense_grad, new_table, new_accum)


def solution(mesh):
    in_specs = (
        P(("dp", "mp"), None, None),
        P(("dp", "mp"), None),
        P(("dp", "mp"), None),
        P(),
        P(("dp", "mp"), None, None),
        P(("dp", "mp"), None),
        P(None, ("dp", "mp"), None),
        P(None, ("dp", "mp")),
    )
    out_specs = (P(("dp", "mp"), None), P(None, ("dp", "mp"), None), P(None, ("dp", "mp")))
    return jax.shard_map(
        per_device, mesh=mesh, in_specs=in_specs, out_specs=out_specs, check_vma=False
    )
```

```python
import jax
import jax.numpy as jnp
import numpy as np
from jax import lax
from jax.experimental import pallas as pl
from jax.experimental.pallas import tpu as pltpu
from jax.sharding import PartitionSpec as P

LEARN_RATE = 0.1
EPSILON = 1e-08


def symmetric_rows(feature_count, wanted):
    row_index, col_index = np.tril_indices(feature_count, -1)
    pair_of = np.full((feature_count, feature_count), -1)
    pair_of[row_index, col_index] = np.arange(row_index.shape[0])
    pair_of[col_index, row_index] = np.arange(row_index.shape[0])
    matrix = np.zeros((len(wanted), feature_count, row_index.shape[0]), np.float32)
    for place, i in enumerate(wanted):
        for j in range(feature_count):
            if 0 <= i < feature_count and i != j:
                matrix[place, j, pair_of[i, j]] = 1.0
    return jnp.asarray(matrix.reshape(-1, row_index.shape[0]), jnp.bfloat16)


def feature_grads(features, top_cot, pair_weight, wanted):
    batch_rows, feature_count, _ = features.shape
    expanded = jnp.dot(
        symmetric_rows(feature_count, wanted), pair_weight, preferred_element_type=jnp.float32
    ).astype(jnp.bfloat16)
    symmetric = jnp.einsum("bh,zh->bz", top_cot, expanded, preferred_element_type=jnp.float32)
    symmetric = symmetric.reshape(batch_rows, len(wanted), feature_count)
    return jnp.einsum("bij,bje->bie", symmetric, features, precision=lax.Precision.HIGH)


def sum_kernel(ids_ref, rows_ref, out_ref):
    sources = rows_ref.shape[0]
    blocks, _, block_rows, width = out_ref.shape
    samples = rows_ref.shape[2]
    base = pl.program_id(1) * (blocks * block_rows)
    target = lax.broadcasted_iota(jnp.int32, (blocks * block_rows, samples), 0) + base
    total = jnp.zeros((blocks * block_rows, width), jnp.float32)
    for s in range(sources):
        onehot = (target == ids_ref[s, 0]).astype(jnp.float32).astype(jnp.bfloat16)
        total = total + jnp.dot(onehot, rows_ref[s, 0], preferred_element_type=jnp.float32)
    out_ref[...] = total.reshape(blocks, 1, block_rows, width).astype(out_ref.dtype)


def sum_rows(ids, rows, blocks, block_rows, dtype):
    sources, tables, samples, width = rows.shape
    step = 4 if blocks % 4 == 0 else 1
    return pl.pallas_call(
        sum_kernel,
        grid=(tables, blocks // step),
        in_specs=[
            pl.BlockSpec((sources, 1, 1, samples), lambda t, h: (0, t, 0, 0)),
            pl.BlockSpec((sources, 1, samples, width), lambda t, h: (0, t, 0, 0)),
        ],
        out_specs=pl.BlockSpec((step, 1, block_rows, width), lambda t, h: (h, t, 0, 0)),
        out_shape=jax.ShapeDtypeStruct((blocks, tables, block_rows, width), dtype),
        cost_estimate=pl.CostEstimate(
            flops=2 * tables * sources * samples * blocks * block_rows * width,
            bytes_accessed=rows.size * 2 + blocks * tables * block_rows * width * 4,
            transcendentals=0,
        ),
    )(ids[:, :, None, :], rows)


def per_device(sparse_vecs, dense_vec, top_cot, top_weight, owner_ids, local_rows, table, accum):
    batch_rows, table_count, row_width = sparse_vecs.shape
    dp_count, mp_count = lax.axis_size("dp"), lax.axis_size("mp")
    rows_own = table.shape[1]
    group_rows = rows_own * mp_count
    per_mp = -(-table_count // mp_count)
    padding = per_mp * mp_count - table_count
    inner = 2 if dp_count % 2 == 0 else 1
    outer = dp_count // inner
    first = (per_mp + 1) // 2
    chunks = [range(first), range(first, per_mp)]

    keys = (owner_ids[:, :, 0] * group_rows + local_rows).T
    keys = jnp.pad(keys, ((0, padding), (0, 0)), constant_values=-1)
    keys = keys.reshape(per_mp, mp_count, batch_rows).transpose(1, 0, 2)
    keys = lax.all_to_all(keys, "mp", split_axis=0, concat_axis=0, tiled=True)
    owner, local = keys // group_rows, keys % group_rows
    place = owner // inner * group_rows + local
    part = owner % inner
    mine = lax.axis_index("dp") % inner
    own_place = jnp.where((keys >= 0) & (part == mine), place, -1)
    other_place = jnp.where((keys >= 0) & (part != mine), place, -1)

    features = jnp.concatenate([dense_vec[:, None, :], sparse_vecs], axis=1).astype(jnp.float32)
    pair_weight = top_weight[row_width:]
    swap = [(i, i ^ 1) for i in range(dp_count)]
    groups = [[r + inner * k for k in range(outer)] for r in range(inner)]
    sums = []
    for chunk in chunks:
        wanted = [1 + k * mp_count + m for m in range(mp_count) for k in chunk]
        last = chunk is chunks[-1]
        grads = feature_grads(features, top_cot, pair_weight, wanted + [0] if last else wanted)
        if last:
            direct = jnp.einsum(
                "bh,zh->bz", top_cot, top_weight[:row_width], preferred_element_type=jnp.float32
            )
            dense_grad = (direct + grads[:, -1]).astype(jnp.bfloat16)
            grads = grads[:, :-1]
        send = grads.astype(jnp.bfloat16).transpose(1, 0, 2)
        rows = lax.all_to_all(
            send.reshape(mp_count, len(chunk), batch_rows, row_width),
            "mp",
            split_axis=0,
            concat_axis=0,
            tiled=True,
        )
        cut = slice(chunk[0], chunk[-1] + 1)
        total = sum_rows(own_place[:, cut], rows, outer, group_rows, jnp.float32)
        if inner == 2:
            other = sum_rows(other_place[:, cut], rows, outer, group_rows, jnp.bfloat16)
            total = total + lax.ppermute(other, "dp", swap).astype(jnp.float32)
        parts = lax.all_to_all(
            total.astype(jnp.bfloat16),
            "dp",
            split_axis=0,
            concat_axis=0,
            axis_index_groups=groups,
            tiled=True,
        )
        sums.append(jnp.sum(parts.astype(jnp.float32), axis=0).astype(jnp.bfloat16))
    summed = jnp.concatenate(sums, axis=0)
    summed = summed.reshape(per_mp, mp_count, rows_own, row_width).transpose(1, 0, 2, 3)
    row_grad = lax.all_to_all(summed, "mp", split_axis=0, concat_axis=0, tiled=True)
    row_grad = row_grad.transpose(1, 0, 2, 3).reshape(per_mp * mp_count, rows_own, row_width)
    row_grad = row_grad[:table_count].astype(jnp.float32)
    new_accum = accum + jnp.mean(row_grad * row_grad, axis=-1)
    new_table = table - LEARN_RATE * row_grad / (jnp.sqrt(new_accum)[:, :, None] + EPSILON)
    return (dense_grad, new_table, new_accum)


def solution(mesh):
    in_specs = (
        P(("dp", "mp"), None, None),
        P(("dp", "mp"), None),
        P(("dp", "mp"), None),
        P(),
        P(("dp", "mp"), None, None),
        P(("dp", "mp"), None),
        P(None, ("dp", "mp"), None),
        P(None, ("dp", "mp")),
    )
    out_specs = (P(("dp", "mp"), None), P(None, ("dp", "mp"), None), P(None, ("dp", "mp")))
    return jax.shard_map(
        per_device, mesh=mesh, in_specs=in_specs, out_specs=out_specs, check_vma=False
    )
```

```python
import jax
import jax.numpy as jnp
import numpy as np
from jax import lax
from jax.experimental import pallas as pl
from jax.experimental.pallas import tpu as pltpu
from jax.sharding import PartitionSpec as P

LEARN_RATE = 0.1
EPSILON = 1e-08


def symmetric_rows(feature_count, wanted):
    row_index, col_index = np.tril_indices(feature_count, -1)
    pair_of = np.full((feature_count, feature_count), -1)
    pair_of[row_index, col_index] = np.arange(row_index.shape[0])
    pair_of[col_index, row_index] = np.arange(row_index.shape[0])
    matrix = np.zeros((len(wanted), feature_count, row_index.shape[0]), np.float32)
    for place, i in enumerate(wanted):
        for j in range(feature_count):
            if 0 <= i < feature_count and i != j:
                matrix[place, j, pair_of[i, j]] = 1.0
    return jnp.asarray(matrix.reshape(-1, row_index.shape[0]), jnp.bfloat16)


def feature_grads(features, top_cot, pair_weight, wanted):
    batch_rows, feature_count, _ = features.shape
    expanded = jnp.dot(
        symmetric_rows(feature_count, wanted), pair_weight, preferred_element_type=jnp.float32
    ).astype(jnp.bfloat16)
    symmetric = jnp.einsum("bh,zh->bz", top_cot, expanded, preferred_element_type=jnp.float32)
    symmetric = symmetric.reshape(batch_rows, len(wanted), feature_count)
    return jnp.einsum("bij,bje->bie", symmetric, features, precision=lax.Precision.HIGH)


def sum_kernel(ids_ref, rows_ref, out_ref):
    sources = rows_ref.shape[0]
    blocks, shares, _, share_rows, width = out_ref.shape
    block_rows = shares * share_rows
    samples = rows_ref.shape[2]
    base = pl.program_id(1) * (blocks * block_rows)
    target = lax.broadcasted_iota(jnp.int32, (blocks * block_rows, samples), 0) + base
    total = jnp.zeros((blocks * block_rows, width), jnp.float32)
    for s in range(sources):
        onehot = (target == ids_ref[s, 0]).astype(jnp.float32).astype(jnp.bfloat16)
        total = total + jnp.dot(onehot, rows_ref[s, 0], preferred_element_type=jnp.float32)
    out_ref[...] = total.reshape(out_ref.shape).astype(out_ref.dtype)


def sum_rows(ids, rows, blocks, shares, share_rows, dtype):
    sources, tables, samples, width = rows.shape
    step = 4 if blocks % 4 == 0 else 1
    return pl.pallas_call(
        sum_kernel,
        grid=(tables, blocks // step),
        in_specs=[
            pl.BlockSpec((sources, 1, 1, samples), lambda t, h: (0, t, 0, 0)),
            pl.BlockSpec((sources, 1, samples, width), lambda t, h: (0, t, 0, 0)),
        ],
        out_specs=pl.BlockSpec(
            (step, shares, 1, share_rows, width), lambda t, h: (h, 0, t, 0, 0)
        ),
        out_shape=jax.ShapeDtypeStruct((blocks, shares, tables, share_rows, width), dtype),
        cost_estimate=pl.CostEstimate(
            flops=2 * tables * sources * samples * blocks * shares * share_rows * width,
            bytes_accessed=rows.size * 2 + blocks * shares * tables * share_rows * width * 4,
            transcendentals=0,
        ),
    )(ids[:, :, None, :], rows)


def per_device(sparse_vecs, dense_vec, top_cot, top_weight, owner_ids, local_rows, table, accum):
    batch_rows, table_count, row_width = sparse_vecs.shape
    dp_count, mp_count = lax.axis_size("dp"), lax.axis_size("mp")
    rows_own = table.shape[1]
    group_rows = rows_own * mp_count
    per_mp = -(-table_count // mp_count)
    padding = per_mp * mp_count - table_count
    inner = 2 if dp_count % 2 == 0 else 1
    outer = dp_count // inner
    first = (per_mp + 1) // 2
    chunks = [range(first), range(first, per_mp)]

    keys = (owner_ids[:, :, 0] * group_rows + local_rows).T
    keys = jnp.pad(keys, ((0, padding), (0, 0)), constant_values=-1)
    keys = keys.reshape(per_mp, mp_count, batch_rows).transpose(1, 0, 2)
    keys = lax.all_to_all(keys, "mp", split_axis=0, concat_axis=0, tiled=True)
    owner, local = keys // group_rows, keys % group_rows
    place = owner // inner * group_rows + local
    part = owner % inner
    mine = lax.axis_index("dp") % inner
    own_place = jnp.where((keys >= 0) & (part == mine), place, -1)
    other_place = jnp.where((keys >= 0) & (part != mine), place, -1)

    features = jnp.concatenate([dense_vec[:, None, :], sparse_vecs], axis=1).astype(jnp.float32)
    pair_weight = top_weight[row_width:]
    swap = [(i, i ^ 1) for i in range(dp_count)]
    groups = [
        [(r + inner * k) * mp_count + m for k in range(outer) for m in range(mp_count)]
        for r in range(inner)
    ]
    sums = []
    for chunk in chunks:
        wanted = [1 + k * mp_count + m for m in range(mp_count) for k in chunk]
        last = chunk is chunks[-1]
        grads = feature_grads(features, top_cot, pair_weight, wanted + [0] if last else wanted)
        if last:
            direct = jnp.einsum(
                "bh,zh->bz", top_cot, top_weight[:row_width], preferred_element_type=jnp.float32
            )
            dense_grad = (direct + grads[:, -1]).astype(jnp.bfloat16)
            grads = grads[:, :-1]
        send = grads.astype(jnp.bfloat16).transpose(1, 0, 2)
        rows = lax.all_to_all(
            send.reshape(mp_count, len(chunk), batch_rows, row_width),
            "mp",
            split_axis=0,
            concat_axis=0,
            tiled=True,
        )
        cut = slice(chunk[0], chunk[-1] + 1)
        total = sum_rows(own_place[:, cut], rows, outer, mp_count, rows_own, jnp.float32)
        if inner == 2:
            other = sum_rows(other_place[:, cut], rows, outer, mp_count, rows_own, jnp.bfloat16)
            total = total + lax.ppermute(other, "dp", swap).astype(jnp.float32)
        parts = lax.all_to_all(
            total.astype(jnp.bfloat16).reshape(
                outer * mp_count, len(chunk), rows_own, row_width
            ),
            ("dp", "mp"),
            split_axis=0,
            concat_axis=0,
            axis_index_groups=groups,
            tiled=True,
        )
        parts = parts.reshape(outer, mp_count, len(chunk), rows_own, row_width)
        summed = jnp.sum(parts.astype(jnp.float32), axis=0).transpose(1, 0, 2, 3)
        sums.append(summed.reshape(len(chunk) * mp_count, rows_own, row_width))
    row_grad = jnp.concatenate(sums, axis=0)[:table_count]
    new_accum = accum + jnp.mean(row_grad * row_grad, axis=-1)
    new_table = table - LEARN_RATE * row_grad / (jnp.sqrt(new_accum)[:, :, None] + EPSILON)
    return (dense_grad, new_table, new_accum)


def solution(mesh):
    in_specs = (
        P(("dp", "mp"), None, None),
        P(("dp", "mp"), None),
        P(("dp", "mp"), None),
        P(),
        P(("dp", "mp"), None, None),
        P(("dp", "mp"), None),
        P(None, ("dp", "mp"), None),
        P(None, ("dp", "mp")),
    )
    out_specs = (P(("dp", "mp"), None), P(None, ("dp", "mp"), None), P(None, ("dp", "mp")))
    return jax.shard_map(
        per_device, mesh=mesh, in_specs=in_specs, out_specs=out_specs, check_vma=False
    )
```
